32 devices in a mesh: tm: 8 (over y, x, core), scen: 4 (over z).
Axes of the slice: x: 2, y: 2, z: 4, core: 2. Of those that a mesh axis runs over, the one named last changes fastest.
Arguments:
- closed_loop: float32 [256, 96, 96], P('tm'), may hold values from -1 to 1
- gains: float32 [256, 48, 96], P('tm'), may hold values from -0.625 to 0.625
- feedforward: float32 [256, 48], P('tm'), may hold values from -6 to 6
- drift_terms: float32 [256, 96], P('tm'), may hold values from -0.3 to 0.3
- initial_states: float32 [96, 256], P(None, ('tm', 'scen')), may hold values from -6 to 6
Outputs:
- states: float32 [256, 96, 256], P(('tm', 'scen'))
- controls: float32 [256, 48, 256], P(('tm', 'scen'))
The draws below stay inside these ranges and needn't reach their ends.
All inputs are finite; a program needn't handle non-finite values.
Results may differ from the reference program's by a relative error of at most 0.0003.
Values sent between devices are 32-bit elements; how exact they have to be, the bound alone decides.
A program may use at most 64 MiB of HBM per device.

```python
import math
import jax
import jax.numpy as jnp
from jax import lax

NX = 96
NU = 48
PERIOD_LENGTH = 256
SCEN = 256


def draw_closed_loop(key, part):
    draw_generator_bases = jax.random.split(jax.random.fold_in(key, 11), 7)
    sluggish_selector = jax.random.uniform(draw_generator_bases[0], (NX,)) < 0.5
    slow_scale = jnp.exp(jax.random.uniform(draw_generator_bases[1], (NX,), minval=math.log(3.0 * PERIOD_LENGTH), maxval=math.log(12.0 * PERIOD_LENGTH)))
    quick_scale = jnp.exp(jax.random.uniform(draw_generator_bases[2], (NX,), minval=math.log(15.0), maxval=math.log(40.0)))
    time_scale = jnp.where(sluggish_selector, slow_scale, quick_scale)
    random_perturbation = jnp.exp(jax.random.uniform(draw_generator_bases[3], (PERIOD_LENGTH, NX), minval=math.log(0.7), maxval=math.log(1.4)))
    decay_speeds = jnp.exp(-1.0 / (time_scale[None, :] * random_perturbation))
    spell_length_total = jax.random.randint(draw_generator_bases[4], (3,), 0, PERIOD_LENGTH)
    interval_persisting = jax.random.uniform(draw_generator_bases[5], (3,), minval=0.5, maxval=0.8)
    concordant_number = jnp.arange(PERIOD_LENGTH)[:, None] == spell_length_total[None, :]
    persistence_markers = jnp.prod(jnp.where(concordant_number, interval_persisting[None, :], 1.0), axis=1)
    decay_speeds = decay_speeds * jnp.where(sluggish_selector[None, :], persistence_markers[:, None], 1.0)
    noise = jax.random.normal(draw_generator_bases[6], (PERIOD_LENGTH, NX, NX), dtype=jnp.float32) * (0.18 / math.sqrt(NX))
    same_group = (sluggish_selector[:, None] == sluggish_selector[None, :]).astype(jnp.float32)
    skewed_portion = (noise - jnp.swapaxes(noise, 1, 2)) / math.sqrt(2.0) * same_group[None, :, :]
    identity_map = jnp.eye(NX, dtype=jnp.float32)[None, :, :]
    rotation = jnp.linalg.solve(identity_map - skewed_portion, identity_map + skewed_portion)
    return (decay_speeds[:, :, None] * rotation).astype(jnp.float32)


def level_of(rng, shape, shards, low, high):
    gain = 1.0
    for position, shards_of in shards:
        steps = jax.random.uniform(jax.random.fold_in(jax.random.fold_in(rng, 6), position), (shards_of,), jnp.float32, low / len(shards), high / len(shards))
        gain = gain * jnp.repeat(jnp.exp(steps), shape[position] // shards_of).reshape((-1,) + (1,) * (len(shape) - 1 - position))
    return gain


def centred(rng, shape, spread, reach, shards=(), kind=jnp.bfloat16):
    result = spread * jax.random.normal(rng, shape, jnp.float32)
    if shards:
        result = result * level_of(rng, shape, shards, -0.22, 0.18)
    return jnp.clip(result, -reach, reach).astype(kind)


def setup_inputs(seed: int = 0) -> dict:
    keys = jax.random.split(jax.random.key(seed), 6)
    closed_loop = draw_closed_loop(jax.random.fold_in(keys[5], 71), 0)
    gains = centred(keys[1], (PERIOD_LENGTH, NU, NX), NX ** -0.5, 0.625, ((0, 8),), jnp.float32)
    feedforward = centred(keys[2], (PERIOD_LENGTH, NU), 1.0, 6.0, ((0, 8),), jnp.float32)
    drift_terms = centred(keys[3], (PERIOD_LENGTH, NX), 0.05, 0.3, ((0, 8),), jnp.float32)
    initial_states = centred(keys[4], (NX, SCEN), 1.0, 6.0, ((1, 32),), jnp.float32)
    return dict(closed_loop=closed_loop, gains=gains, feedforward=feedforward, drift_terms=drift_terms, initial_states=initial_states)


def reference(closed_loop, gains, feedforward, drift_terms, initial_states):
    highest = lax.Precision.HIGHEST

    def advance(state, inputs):
        matrix, gain_rows, feed_term, drift_term = inputs
        control = feed_term[:, None] - jnp.dot(gain_rows.astype(jnp.float32), state.astype(jnp.float32), precision=highest, preferred_element_type=jnp.float32)
        next_state = jnp.dot(matrix.astype(jnp.float32), state.astype(jnp.float32), precision=highest, preferred_element_type=jnp.float32) + drift_term[:, None]
        return (next_state, (state, control))
    start = initial_states.astype(jnp.float32)
    _, (state_path, control_path) = lax.scan(advance, start, (closed_loop, gains, feedforward, drift_terms))
    return (jnp.transpose(state_path, (2, 1, 0)), jnp.transpose(control_path, (2, 1, 0)))
```

```python
import functools
import jax
import jax.numpy as jnp
from jax import lax
from jax.experimental import pallas as pl
from jax.experimental.pallas import tpu as pltpu
from jax.sharding import PartitionSpec as P

LANES = 128
MESH = pl.DeviceIdType.MESH
f32 = jnp.float32
bf16 = jnp.bfloat16


def up(value, unit):
    return -(-value // unit) * unit


def split(value):
    high = value.astype(bf16)
    low = (value - high.astype(f32)).astype(bf16)
    return jnp.concatenate([high, low], axis=1)


def product(left, right):
    wide = right.shape[1] // 2
    both = jnp.concatenate([right, right], axis=0)
    out = jnp.dot(left, both, preferred_element_type=f32)
    return out[:, :wide] + out[:, wide:]


def stack_rows(rows):
    high = rows.astype(bf16)
    low = (rows - high.astype(f32)).astype(bf16)
    return jnp.concatenate(
        [jnp.concatenate([high, high], axis=1), jnp.concatenate([low, low], axis=1)], axis=0
    )


def apply_rows(stacked, maps):
    out = lax.dot_general(
        stacked, maps, (((1,), (1,)), ((), ())), preferred_element_type=f32
    )
    half = out.shape[0] // 2
    return out[:half] + out[half:]


def rollout_kernel(
    n, nx, nu, tl, sl,
    a_hbm, k_hbm, ff_hbm, d_hbm, x0_hbm, x_tile, u_tile,
    a_ref, k_ref, ff_ref, d_ref, x0_ref,
    leaf, nodes, pre, wf, tile, x_send, x_all, t_send, t_recv, p_send, p_recv, send, recv,
    in_sem, x_ssem, x_rsem, t_ssem, t_rsem, p_ssem, p_rsem, o_ssem, o_rsem,
):
    D = tile.shape[0]
    dr = t_send.shape[0]
    rows = nx + nu
    pairs = n // 2
    me = lax.axis_index("tm")
    pair, odd = me // 2, me % 2

    loads = [
        pltpu.make_async_copy(src, dst, in_sem.at[i])
        for i, (src, dst) in enumerate(
            ((d_hbm, d_ref), (a_hbm, a_ref), (x0_hbm, x0_ref), (ff_hbm, ff_ref), (k_hbm, k_ref))
        )
    ]
    for load in loads:
        load.start()
    barrier = pltpu.get_barrier_semaphore()
    for k in range(1, n):
        pl.semaphore_signal(
            barrier, inc=1, device_id={"tm": (me + k) % n}, device_id_type=MESH
        )

    lane = lax.broadcasted_iota(jnp.int32, (D, D), 1)
    row = lax.broadcasted_iota(jnp.int32, (D, D), 0)
    corner = jnp.where((lane == nx) & (row == nx), 1.0, 0.0).astype(f32)

    tile[...] = jnp.zeros((D, D), f32)
    loads[0].wait()
    tile[0:tl, 0:nx] = d_ref[...]
    d_cols = jnp.transpose(tile[...])
    side = jnp.zeros((nx, D - nx), f32)
    side_u = jnp.zeros((nu, D - nx), f32)
    loads[1].wait()
    foot = jnp.zeros((D - nx, D), f32)

    def make_leaf(t):
        a = jnp.concatenate([jnp.concatenate([a_ref[t], side], axis=1), foot], axis=0)
        a = jnp.where(lane == nx, pltpu.roll(d_cols, nx - t, 1), a) + corner
        leaf[t, 0:D] = split(a)

    for t in range(tl):
        make_leaf(t)

    def node(level, k):
        if level == 0:
            return leaf[k, 0:D]
        return nodes[tl - 2 * (tl >> level) + k]

    levels = tl.bit_length() - 1
    root = None
    batch = 4
    for level in range(1, levels + 1):
        count = tl >> level

        for first in range(0, count, batch):
            group = range(first, min(count, first + batch))
            values = [product(node(level - 1, 2 * k + 1), node(level - 1, 2 * k)) for k in group]
            if level == levels:
                root = values[0]
                break
            for k, value in zip(group, values):
                nodes[tl - 2 * (tl >> level) + k] = split(value)
    root_split = split(root)
    t_send[...] = root[:dr]

    pl.semaphore_wait(barrier, n - 1)

    loads[2].wait()
    x_rows = jnp.concatenate([x0_ref[...], jnp.zeros((sl, D - nx), f32)], axis=1)
    x_rows = jnp.where(lax.broadcasted_iota(jnp.int32, (sl, D), 1) == nx, 1.0, x_rows)
    x_send[...] = x_rows
    x_all[me] = x_rows

    def x_copy(src, dst):
        return pltpu.make_async_remote_copy(
            src_ref=x_send, dst_ref=x_all.at[src],
            send_sem=x_ssem.at[dst], recv_sem=x_rsem.at[src],
            device_id={"tm": dst}, device_id_type=MESH,
        )

    t_copy = pltpu.make_async_remote_copy(
        src_ref=t_send, dst_ref=t_recv, send_sem=t_ssem, recv_sem=t_rsem,
        device_id={"tm": me + 1 - 2 * odd}, device_id_type=MESH,
    )

    @pl.when(odd == 0)
    def _():
        t_copy.start()

    for k in range(1, n):
        x_copy(me, (me + k) % n).start()

    loads[3].wait()
    tile[...] = jnp.zeros((D, D), f32)
    tile[0:tl, 0:nu] = ff_ref[...]
    f_cols = jnp.transpose(tile[...])[:nu]
    lane_u = lax.broadcasted_iota(jnp.int32, (nu, D), 1)
    loads[4].wait()

    def make_gain(t):
        g = -jnp.concatenate([k_ref[t], side_u], axis=1)
        g = jnp.where(lane_u == nx, pltpu.roll(f_cols, nx - t, 1), g)
        leaf[t, D : D + nu] = split(g)

    for t in range(tl):
        make_gain(t)

    eye = jnp.where((lane == row) & (lane <= nx), 1.0, 0.0).astype(f32)
    pre[0] = split(eye)
    wf[pl.ds(0, nx, stride=tl), :] = eye[:nx]

    def put_pre(t, value):
        pre[t] = split(value)
        wf[pl.ds(t, nx, stride=tl), :] = value[:nx]

    def p_copy(src_pair, dst):
        return pltpu.make_async_remote_copy(
            src_ref=p_send, dst_ref=p_recv.at[src_pair],
            send_sem=p_ssem.at[dst], recv_sem=p_rsem.at[src_pair],
            device_id={"tm": dst}, device_id_type=MESH,
        )

    pad_rows = jnp.zeros((D - dr, D), f32)

    def full(value):
        return split(jnp.concatenate([value, pad_rows], axis=0))

    def pass_pair():
        @pl.when(odd == 1)
        def _():
            t_copy.wait_recv()
            p_send[...] = product(root_split, full(t_recv[...]))[:dr]

            def go(j, c):
                p_copy(pair, n + 2 * pair + 1 - j).start()
                return c

            lax.fori_loop(2 * pair + 2, n, go, 0)

    for level in range(levels - 1, 0, -1):
        size = 1 << level
        put_first = nodes[tl - 2 * (tl >> level)]
        pre[size] = put_first
        wf[pl.ds(size, nx, stride=tl), :] = (
            put_first[:nx, :D].astype(f32) + put_first[:nx, D:].astype(f32)
        )
        count = (tl >> (level + 1)) - 1

        for first in range(0, count, batch):
            group = [2 * (j + 1) for j in range(first, min(count, first + batch))]
            values = [product(node(level, k), pre[size * k]) for k in group]
            for k, value in zip(group, values):
                put_pre(size * (k + 1), value)
        if level == min(2, levels - 1):
            pass_pair()

    for first in range(0, tl, 2 * batch):
        group = range(first, min(tl, first + 2 * batch), 2)
        values = [product(leaf[t], pre[t]) for t in group]
        for t, value in zip(group, values):
            put_pre(t + 1, value[:D])
            wf[pl.ds(nx * tl + t, nu, stride=tl), :] = value[D:]
        values = [product(leaf[t + 1, D : D + nu], pre[t + 1]) for t in group]
        for t, value in zip(group, values):
            wf[pl.ds(nx * tl + t + 1, nu, stride=tl), :] = value

    for k in range(1, n):
        x_copy((me + k) % n, me).wait_recv()
    entry = jnp.concatenate([x_all[k] for k in range(n)], axis=0)

    def chain(p, entry):
        p_copy(p, me).wait_recv()
        return apply_rows(stack_rows(entry), full(p_recv[p]))

    entry = lax.fori_loop(0, pair, chain, entry)
    partner = jnp.where(odd == 1, t_recv[...], eye[:dr])
    entry = apply_rows(stack_rows(entry), full(partner))
    stacked = stack_rows(entry)

    chunks = o_ssem.shape[1]
    span = rows * tl // chunks

    def o_copy(src, dst, c):
        return pltpu.make_async_remote_copy(
            src_ref=send.at[dst, :, pl.ds(c * span, span)],
            dst_ref=recv.at[src, :, pl.ds(c * span, span)],
            send_sem=o_ssem.at[dst, c], recv_sem=o_rsem.at[src, c],
            device_id={"tm": dst}, device_id_type=MESH,
        )

    for c in range(chunks):
        here = slice(c * span, (c + 1) * span)
        part = apply_rows(stacked, split(wf[here, :]))
        for d in range(n):
            send[d, :, here] = part[d * sl : (d + 1) * sl]
        recv[me, :, here] = send[me, :, here]
        for k in range(1, n):
            o_copy(me, (me + k) % n, c).start()

    for k in range(1, n):
        x_copy(me, (me + k) % n).wait_send()

    @pl.when(odd == 0)
    def _():
        t_copy.wait_send()

    @pl.when(odd == 1)
    def _():
        def done(dst, c):
            p_copy(pair, dst).wait_send()
            return c

        lax.fori_loop(2 * pair + 2, n, done, 0)

    group = LANES // tl
    place = lax.broadcasted_iota(jnp.int32, (sl, LANES), 1) // tl
    per = LANES // tl
    for c in range(chunks):
        for h in range(n // group):
            for b in range(group):
                src = h * group + b

                @pl.when(src != me)
                def _(src=src, c=c):
                    o_copy(src, me, c).wait_recv()

            for q in range(c * span // LANES, (c + 1) * span // LANES):
                parts = [
                    recv[h * group + b, :, q * LANES : (q + 1) * LANES] for b in range(group)
                ]
                for i in range(per):
                    value = None
                    for b in range(group):
                        shift = ((b - i) * tl) % LANES
                        moved = pltpu.roll(parts[b], shift, 1) if shift else parts[b]
                        value = moved if value is None else jnp.where(place == b, moved, value)
                    index = q * per + i
                    if index < nx:
                        x_tile[h, pl.ds(index, sl, stride=nx), :] = value
                    else:
                        u_tile[h, pl.ds(index - nx, sl, stride=nu), :] = value

    for c in range(chunks):
        for k in range(1, n):
            o_copy(me, (me + k) % n, c).wait_send()


def store_kernel(halves, x_ref, u_ref, states_hbm, controls_hbm, sem):
    copies = [
        pltpu.make_async_copy(
            src.at[h], dst.at[:, :, pl.ds(h * LANES, LANES)], sem.at[i, h]
        )
        for i, (src, dst) in enumerate(((x_ref, states_hbm), (u_ref, controls_hbm)))
        for h in range(halves)
    ]
    for copy in copies:
        copy.start()
    for copy in copies:
        copy.wait()


def body(closed_loop, gains, feedforward, drift_terms, initial_states):
    tl, nx = closed_loop.shape[:2]
    nu = gains.shape[1]
    sl = initial_states.shape[1]
    n = lax.axis_size("tm")
    D = up(nx + 1, LANES)
    dr = up(nx + 1, 8)
    rows = nx + nu
    vmem = pl.BlockSpec(memory_space=pltpu.VMEM)
    dma = pltpu.SemaphoreType.DMA
    hbm = pl.BlockSpec(memory_space=pltpu.HBM)
    chunks = rows * tl // (4 * LANES) if rows * tl % (4 * LANES) == 0 else 1
    steps = n * tl
    halves = steps // LANES
    x_tile, u_tile = pl.pallas_call(
        functools.partial(rollout_kernel, n, nx, nu, tl, sl),
        out_shape=(
            jax.ShapeDtypeStruct((halves, sl * nx, LANES), f32),
            jax.ShapeDtypeStruct((halves, sl * nu, LANES), f32),
        ),
        in_specs=[hbm] * 5,
        out_specs=(vmem, vmem),
        scratch_shapes=[
            pltpu.VMEM((tl, nx, nx), f32),
            pltpu.VMEM((tl, nu, nx), f32),
            pltpu.VMEM((tl, nu), f32),
            pltpu.VMEM((tl, nx), f32),
            pltpu.VMEM((sl, nx), f32),
            pltpu.VMEM((tl, D + nu, 2 * D), bf16),
            pltpu.VMEM((tl, D, 2 * D), bf16),
            pltpu.VMEM((tl, D, 2 * D), bf16),
            pltpu.VMEM((rows * tl, D), f32),
            pltpu.VMEM((D, D), f32),
            pltpu.VMEM((sl, D), f32),
            pltpu.VMEM((n, sl, D), f32),
            pltpu.VMEM((dr, D), f32),
            pltpu.VMEM((dr, D), f32),
            pltpu.VMEM((dr, D), f32),
            pltpu.VMEM((n // 2, dr, D), f32),
            pltpu.VMEM((n, sl, rows * tl), f32),
            pltpu.VMEM((n, sl, rows * tl), f32),
            dma((5,)),
            dma((n,)), dma((n,)), dma, dma, dma((n,)), dma((n // 2,)),
            dma((n, chunks)), dma((n, chunks)),
        ],
        compiler_params=pltpu.CompilerParams(
            collective_id=0, has_side_effects=True, vmem_limit_bytes=48 * 2**20
        ),
    )(
        *(
            pltpu.with_memory_space_constraint(value, pltpu.HBM)
            for value in (closed_loop, gains, feedforward, drift_terms, initial_states.T)
        )
    )
    return pl.pallas_call(
        functools.partial(store_kernel, halves),
        out_shape=(
            jax.ShapeDtypeStruct((sl, nx, steps), f32),
            jax.ShapeDtypeStruct((sl, nu, steps), f32),
        ),
        in_specs=[vmem] * 2,
        out_specs=(hbm, hbm),
        scratch_shapes=[dma((2, halves))],
        compiler_params=pltpu.CompilerParams(vmem_limit_bytes=2**20),
    )(x_tile.reshape(halves, sl, nx, LANES), u_tile.reshape(halves, sl, nu, LANES))


def solution(mesh):
    return jax.shard_map(
        body,
        mesh=mesh,
        in_specs=(
            P("tm", None, None),
            P("tm", None, None),
            P("tm", None),
            P("tm", None),
            P(None, ("tm", "scen")),
        ),
        out_specs=(P(("tm", "scen"), None, None), P(("tm", "scen"), None, None)),
        check_vma=False,
    )
```

```python
import functools
import jax
import jax.numpy as jnp
from jax import lax
from jax.experimental import pallas as pl
from jax.experimental.pallas import tpu as pltpu
from jax.sharding import PartitionSpec as P

LANES = 128
SIZES = (3, 3)
SOON = 7
PIECES = 1
BATCH = 4
WIDE = 8
MESH = pl.DeviceIdType.MESH
f32 = jnp.float32
bf16 = jnp.bfloat16


def spans(total, unit):
    left, edges = total // unit, [0]
    for size in SIZES:
        if size < left:
            left -= size
            edges.append(edges[-1] + size * unit)
    return list(zip(edges, edges[1:] + [total]))


def order(me, n):
    if n != 8:
        return [(me + k) % n for k in range(1, n)]
    table = []
    for m in range(n):
        pair = m // 2
        first, last = {0: (2, 1), 1: (3, 2), 2: (3, 1), 3: (1, 2)}[pair]
        rest = [2 * first, 2 * first + 1] + [1] * (pair > 0) + [2 * last, 2 * last + 1]
        row = [0] * (pair > 0) + [m + 1 - 2 * (m % 2)] + rest
        table.append(row + [6, 7] * (pair == 0))
    return [
        functools.reduce(lambda acc, m: jnp.where(me == m, table[m][k], acc), range(n), 0)
        for k in range(n - 1)
    ]


def exchange(values, tl):
    group = len(values)
    lane = lax.broadcasted_iota(jnp.int32, values[0].shape, 1) // tl
    gap = group // 2
    while gap:
        low = (lane // gap) % 2 == 0
        out = list(values)
        for i in range(group):
            if (i // gap) % 2 == 0:
                a, b = values[i], values[i + gap]
                out[i] = jnp.where(low, a, pltpu.roll(b, gap * tl, 1))
                out[i + gap] = jnp.where(low, pltpu.roll(a, LANES - gap * tl, 1), b)
        values = out
        gap //= 2
    return values


def up(value, unit):
    return -(-value // unit) * unit


def split(value):
    high = value.astype(bf16)
    low = (value - high.astype(f32)).astype(bf16)
    return jnp.concatenate([high, low], axis=1)


def product(left, right):
    wide = right.shape[1] // 2
    both = jnp.concatenate([right, right], axis=0)
    out = jnp.dot(left, both, preferred_element_type=f32)
    return out[:, :wide] + out[:, wide:]


def stack_rows(rows):
    high = rows.astype(bf16)
    low = (rows - high.astype(f32)).astype(bf16)
    return jnp.concatenate(
        [jnp.concatenate([high, high], axis=1), jnp.concatenate([low, low], axis=1)], axis=0
    )


def apply_rows(stacked, maps):
    out = lax.dot_general(
        stacked, maps, (((1,), (1,)), ((), ())), preferred_element_type=f32
    )
    half = out.shape[0] // 2
    return out[:half] + out[half:]


def rollout_kernel(
    n, nx, nu, tl, sl,
    a_hbm, k_hbm, ff_hbm, d_hbm, x0_hbm, x_tile, u_tile,
    a_ref, k_ref, ff_ref, d_ref, x0_ref,
    leaf, nodes, pre, wf, tile, x_send, x_all, t_send, t_recv, p_send, m_recv, e_send, e_recv, send, recv,
    in_sem, x_ssem, x_rsem, t_ssem, t_rsem, e_ssem, e_rsem, m_ssem, m_rsem, p_ssem, o_ssem, o_rsem,
):
    D = tile.shape[0]
    dr = t_send.shape[0]
    rows = nx + nu
    pairs = n // 2
    me = lax.axis_index("tm")
    pair, odd = me // 2, me % 2

    pieces = PIECES if tl % PIECES == 0 else 1
    some = tl // pieces

    def load(src, dst, i):
        return pltpu.make_async_copy(src, dst, in_sem.at[i])

    a_loads = [
        load(a_hbm.at[pl.ds(i * some, some)], a_ref.at[pl.ds(i * some, some)], 4 + i)
        for i in range(pieces)
    ]
    d_load, x_load = load(d_hbm, d_ref, 0), load(x0_hbm, x0_ref, 1)
    f_load, k_load = load(ff_hbm, ff_ref, 2), load(k_hbm, k_ref, 3)
    for copy in (d_load, *a_loads, x_load, f_load):
        copy.start()
    barrier = pltpu.get_barrier_semaphore()
    for k in range(1, n):
        pl.semaphore_signal(
            barrier, inc=1, device_id={"tm": (me + k) % n}, device_id_type=MESH
        )

    lane = lax.broadcasted_iota(jnp.int32, (D, D), 1)
    row = lax.broadcasted_iota(jnp.int32, (D, D), 0)
    corner = jnp.where((lane == nx) & (row == nx), 1.0, 0.0).astype(f32)

    tile[...] = jnp.zeros((D, D), f32)
    d_load.wait()
    tile[0:tl, 0:nx] = d_ref[...]
    d_cols = jnp.transpose(tile[...])
    side = jnp.zeros((nx, D - nx), f32)
    side_u = jnp.zeros((nu, D - nx), f32)
    foot = jnp.zeros((D - nx, D), f32)

    def make_leaf(t):
        a = jnp.concatenate([jnp.concatenate([a_ref[t], side], axis=1), foot], axis=0)
        a = jnp.where(lane == nx, pltpu.roll(d_cols, nx - t, 1), a) + corner
        leaf[t, 0:D] = split(a)

    def node(level, k):
        if level == 0:
            return leaf[k, 0:D]
        return nodes[tl - 2 * (tl >> level) + k]

    levels = tl.bit_length() - 1
    root = None
    batch = BATCH

    def climb(level, first, last):
        for start in range(first, last, batch):
            group = range(start, min(last, start + batch))
            values = [product(node(level - 1, 2 * k + 1), node(level - 1, 2 * k)) for k in group]
            if level == levels:
                return values[0]
            for k, value in zip(group, values):
                nodes[tl - 2 * (tl >> level) + k] = split(value)

    for i, copy in enumerate(a_loads):
        copy.wait()
        if i == pieces - 1:
            k_load.start()
        for t in range(i * some, (i + 1) * some):
            make_leaf(t)
        if some % 2 == 0:
            root = climb(1, i * some // 2, (i + 1) * some // 2)
    for level in range(1 if some % 2 else 2, levels + 1):
        root = climb(level, 0, tl >> level)
    root_split = split(root)
    t_send[...] = root[:dr]

    pl.semaphore_wait(barrier, n - 1)

    x_load.wait()
    x_rows = jnp.concatenate([x0_ref[...], jnp.zeros((sl, D - nx), f32)], axis=1)
    x_rows = jnp.where(lax.broadcasted_iota(jnp.int32, (sl, D), 1) == nx, 1.0, x_rows)
    x_send[...] = x_rows
    x_all[me] = x_rows

    def x_copy(src, k):
        return pltpu.make_async_remote_copy(
            src_ref=x_send, dst_ref=x_all.at[src],
            send_sem=x_ssem.at[k], recv_sem=x_rsem.at[src],
            device_id={"tm": 2 * ((pair + k) % pairs) + 1}, device_id_type=MESH,
        )

    def to_partner(src, dst, ssem, rsem):
        return pltpu.make_async_remote_copy(
            src_ref=src, dst_ref=dst, send_sem=ssem, recv_sem=rsem,
            device_id={"tm": me + 1 - 2 * odd}, device_id_type=MESH,
        )

    t_copy = to_partner(t_send, t_recv, t_ssem, t_rsem)
    e_copy = to_partner(e_send, e_recv, e_ssem, e_rsem)
    def m_copy(src, slot, dst, ssem):
        return pltpu.make_async_remote_copy(
            src_ref=src, dst_ref=m_recv.at[slot], send_sem=ssem, recv_sem=m_rsem.at[slot],
            device_id={"tm": 2 * dst + 1}, device_id_type=MESH,
        )

    def go(q, c):
        m_copy(t_send, me, q, m_ssem.at[q]).start()
        return c

    lax.fori_loop(pair + 1, pairs - 1, go, 0)
    t_copy.start()
    for k in range(1, pairs):
        x_copy(me, k).start()

    @pl.when(odd == 0)
    def _():
        x_copy(me, 0).start()

    f_load.wait()
    tile[...] = jnp.zeros((D, D), f32)
    tile[0:tl, 0:nu] = ff_ref[...]
    f_cols = jnp.transpose(tile[...])[:nu]
    lane_u = lax.broadcasted_iota(jnp.int32, (nu, D), 1)
    k_load.wait()

    def make_gain(t):
        g = -jnp.concatenate([k_ref[t], side_u], axis=1)
        g = jnp.where(lane_u == nx, pltpu.roll(f_cols, nx - t, 1), g)
        leaf[t, D : D + nu] = split(g)

    for t in range(tl):
        make_gain(t)

    eye = jnp.where((lane == row) & (lane <= nx), 1.0, 0.0).astype(f32)
    pre[0] = split(eye)
    wf[pl.ds(0, nx, stride=tl), :] = eye[:nx]

    def put_pre(t, value):
        pre[t] = split(value)
        wf[pl.ds(t, nx, stride=tl), :] = value[:nx]

    pad_rows = corner[dr:]

    def full(value):
        return split(jnp.concatenate([value, pad_rows], axis=0))

    passes = (odd == 0) & (pair + 1 < pairs)
    p_copy = m_copy(p_send, pair, pairs - 1, p_ssem)

    def pass_pair():
        @pl.when(passes)
        def _():
            t_copy.wait_recv()
            p_send[...] = product(full(t_recv[...]), root_split)[:dr]
            p_copy.start()

        @pl.when((odd == 0) & (pair + 1 == pairs))
        def _():
            t_copy.wait_recv()

    for level in range(levels - 1, 0, -1):
        size = 1 << level
        put_first = nodes[tl - 2 * (tl >> level)]
        pre[size] = put_first
        wf[pl.ds(size, nx, stride=tl), :] = (
            put_first[:nx, :D].astype(f32) + put_first[:nx, D:].astype(f32)
        )
        count = (tl >> (level + 1)) - 1

        for first in range(0, count, batch):
            group = [2 * (j + 1) for j in range(first, min(count, first + batch))]
            values = [product(node(level, k), pre[size * k]) for k in group]
            for k, value in zip(group, values):
                put_pre(size * (k + 1), value)
        if level == min(2, levels - 1):
            pass_pair()

    for first in range(0, tl, 2 * WIDE):
        group = range(first, min(tl, first + 2 * WIDE), 2)
        values = [product(leaf[t], pre[t]) for t in group]
        for t, value in zip(group, values):
            put_pre(t + 1, value[:D])
            wf[pl.ds(nx * tl + t, nu, stride=tl), :] = value[D:]
        values = [product(leaf[t + 1, D : D + nu], pre[t + 1]) for t in group]
        for t, value in zip(group, values):
            wf[pl.ds(nx * tl + t + 1, nu, stride=tl), :] = value

    @pl.when(odd == 1)
    def _():
        for k in range(1, n):
            x_copy((me + k) % n, 0).wait_recv()
        entry = jnp.concatenate([x_all[k] for k in range(n)], axis=0)

        def chain(k, entry):
            m_copy(t_send, k, pair, p_ssem).wait_recv()
            return apply_rows(stack_rows(entry), full(m_recv[k]))

        count = jnp.where(pair == pairs - 1, pair, 2 * pair)
        entry = lax.fori_loop(0, count, chain, entry)
        e_send[...] = entry
        e_copy.start()
        t_copy.wait_recv()
        e_recv[...] = apply_rows(stack_rows(entry), full(t_recv[...]))

    @pl.when(odd == 0)
    def _():
        e_copy.wait_recv()

    entry = e_recv[...]
    stacked = stack_rows(entry)

    chunks = spans(rows * tl, 4 * LANES)

    def o_copy(src, dst, c):
        start, stop = chunks[c]
        part = pl.ds(start, stop - start)
        return pltpu.make_async_remote_copy(
            src_ref=send.at[dst, :, part], dst_ref=recv.at[src, :, part],
            send_sem=o_ssem.at[dst, c], recv_sem=o_rsem.at[src, c],
            device_id={"tm": dst}, device_id_type=MESH,
        )

    peers = order(me, n)
    soon = SOON
    for c, (start, stop) in enumerate(chunks):
        for first in range(start, stop, 4 * LANES):
            here = slice(first, first + 4 * LANES)
            part = apply_rows(stacked, split(wf[here, :]))
            for d in range(n):
                send[d, :, here] = part[d * sl : (d + 1) * sl]
        recv[me, :, start:stop] = send[me, :, start:stop]
        for dst in peers[:soon]:
            o_copy(me, dst, c).start()
    for dst in peers[soon:]:
        for c in range(len(chunks)):
            o_copy(me, dst, c).start()

    t_copy.wait_send()
    for k in range(1, pairs):
        x_copy(me, k).wait_send()

    @pl.when(odd == 0)
    def _():
        x_copy(me, 0).wait_send()

    def done(q, c):
        m_copy(t_send, me, q, m_ssem.at[q]).wait_send()
        return c

    lax.fori_loop(pair + 1, pairs - 1, done, 0)

    @pl.when(passes)
    def _():
        p_copy.wait_send()

    @pl.when(odd == 1)
    def _():
        e_copy.wait_send()

    group = LANES // tl
    for c, (start, stop) in enumerate(chunks):
        for h in range(n // group):
            for b in range(group):
                src = h * group + b

                @pl.when(src != me)
                def _(src=src, c=c):
                    o_copy(src, me, c).wait_recv()

            for q in range(start // LANES, stop // LANES):
                values = exchange(
                    [recv[h * group + b, :, q * LANES : (q + 1) * LANES] for b in range(group)], tl
                )
                for i, value in enumerate(values):
                    index = q * group + i
                    if index < nx:
                        x_tile[h, pl.ds(index, sl, stride=nx), :] = value
                    else:
                        u_tile[h, pl.ds(index - nx, sl, stride=nu), :] = value

    for c in range(len(chunks)):
        for k in range(1, n):
            o_copy(me, (me + k) % n, c).wait_send()


def store_kernel(halves, x_ref, u_ref, states_hbm, controls_hbm, sem):
    copies = [
        pltpu.make_async_copy(
            src.at[h], dst.at[:, :, pl.ds(h * LANES, LANES)], sem.at[i, h]
        )
        for i, (src, dst) in enumerate(((x_ref, states_hbm), (u_ref, controls_hbm)))
        for h in range(halves)
    ]
    for copy in copies:
        copy.start()
    for copy in copies:
        copy.wait()


def body(closed_loop, gains, feedforward, drift_terms, initial_states):
    tl, nx = closed_loop.shape[:2]
    nu = gains.shape[1]
    sl = initial_states.shape[1]
    n = lax.axis_size("tm")
    D = up(nx + 1, LANES)
    dr = up(nx, 8)
    rows = nx + nu
    vmem = pl.BlockSpec(memory_space=pltpu.VMEM)
    dma = pltpu.SemaphoreType.DMA
    hbm = pl.BlockSpec(memory_space=pltpu.HBM)
    chunks = len(spans(rows * tl, 4 * LANES))
    steps = n * tl
    halves = steps // LANES
    x_tile, u_tile = pl.pallas_call(
        functools.partial(rollout_kernel, n, nx, nu, tl, sl),
        out_shape=(
            jax.ShapeDtypeStruct((halves, sl * nx, LANES), f32),
            jax.ShapeDtypeStruct((halves, sl * nu, LANES), f32),
        ),
        in_specs=[hbm] * 5,
        out_specs=(vmem, vmem),
        scratch_shapes=[
            pltpu.VMEM((tl, nx, nx), f32),
            pltpu.VMEM((tl, nu, nx), f32),
            pltpu.VMEM((tl, nu), f32),
            pltpu.VMEM((tl, nx), f32),
            pltpu.VMEM((sl, nx), f32),
            pltpu.VMEM((tl, D + nu, 2 * D), bf16),
            pltpu.VMEM((tl, D, 2 * D), bf16),
            pltpu.VMEM((tl, D, 2 * D), bf16),
            pltpu.VMEM((rows * tl, D), f32),
            pltpu.VMEM((D, D), f32),
            pltpu.VMEM((sl, D), f32),
            pltpu.VMEM((n, sl, D), f32),
            pltpu.VMEM((dr, D), f32),
            pltpu.VMEM((dr, D), f32),
            pltpu.VMEM((dr, D), f32),
            pltpu.VMEM((n, dr, D), f32),
            pltpu.VMEM((n * sl, D), f32),
            pltpu.VMEM((n * sl, D), f32),
            pltpu.VMEM((n, sl, rows * tl), f32),
            pltpu.VMEM((n, sl, rows * tl), f32),
            dma((4 + 4,)),
            dma((n // 2,)), dma((n,)), dma, dma, dma, dma,
            dma((n // 2,)), dma((n,)), dma,
            dma((n, chunks)), dma((n, chunks)),
        ],
        compiler_params=pltpu.CompilerParams(
            collective_id=0, has_side_effects=True, vmem_limit_bytes=48 * 2**20
        ),
    )(
        *(
            pltpu.with_memory_space_constraint(value, pltpu.HBM)
            for value in (closed_loop, gains, feedforward, drift_terms, initial_states.T)
        )
    )
    return pl.pallas_call(
        functools.partial(store_kernel, halves),
        out_shape=(
            jax.ShapeDtypeStruct((sl, nx, steps), f32),
            jax.ShapeDtypeStruct((sl, nu, steps), f32),
        ),
        in_specs=[vmem] * 2,
        out_specs=(hbm, hbm),
        scratch_shapes=[dma((2, halves))],
        compiler_params=pltpu.CompilerParams(vmem_limit_bytes=2**20),
    )(x_tile.reshape(halves, sl, nx, LANES), u_tile.reshape(halves, sl, nu, LANES))


def solution(mesh):
    return jax.shard_map(
        body,
        mesh=mesh,
        in_specs=(
            P("tm", None, None),
            P("tm", None, None),
            P("tm", None),
            P("tm", None),
            P(None, ("tm", "scen")),
        ),
        out_specs=(P(("tm", "scen"), None, None), P(("tm", "scen"), None, None)),
        check_vma=False,
    )
```

```python
import functools
import jax
import jax.numpy as jnp
from jax import lax
from jax.experimental import pallas as pl
from jax.experimental.pallas import tpu as pltpu
from jax.sharding import PartitionSpec as P

LANES = 128
SIZES = (3, 3)
BATCH = 4
WIDE = 8
MESH = pl.DeviceIdType.MESH
f32 = jnp.float32
bf16 = jnp.bfloat16


def spans(total, unit):
    left, edges = total // unit, [0]
    for size in SIZES:
        if size < left:
            left -= size
            edges.append(edges[-1] + size * unit)
    return list(zip(edges, edges[1:] + [total]))


def order(me, n):
    if n != 8:
        return [(me + k) % n for k in range(1, n)]
    rows = ((1, 0, 2, 3), (0, 1, 3, 2), (0, 2, 1, 3), (0, 3, 1, 2))
    table = [[2 * p + d if p != m // 2 else m + 1 - 2 * (m % 2) for p in rows[m // 2] for d in range(1 + (p != m // 2))] for m in range(n)]
    return [
        functools.reduce(lambda acc, m: jnp.where(me == m, table[m][k], acc), range(n), 0)
        for k in range(n - 1)
    ]


def exchange(values, tl):
    group = len(values)
    lane = lax.broadcasted_iota(jnp.int32, values[0].shape, 1) // tl
    gap = group // 2
    while gap:
        low = (lane // gap) % 2 == 0
        out = list(values)
        for i in range(group):
            if (i // gap) % 2 == 0:
                a, b = values[i], values[i + gap]
                out[i] = jnp.where(low, a, pltpu.roll(b, gap * tl, 1))
                out[i + gap] = jnp.where(low, pltpu.roll(a, LANES - gap * tl, 1), b)
        values = out
        gap //= 2
    return values


def up(value, unit):
    return -(-value // unit) * unit


def split(value):
    high = value.astype(bf16)
    low = (value - high.astype(f32)).astype(bf16)
    return jnp.concatenate([high, low], axis=1)


def product(left, right):
    wide = right.shape[1] // 2
    both = jnp.concatenate([right, right], axis=0)
    out = jnp.dot(left, both, preferred_element_type=f32)
    return out[:, :wide] + out[:, wide:]


def stack_rows(rows):
    high = rows.astype(bf16)
    low = (rows - high.astype(f32)).astype(bf16)
    return jnp.concatenate(
        [jnp.concatenate([high, high], axis=1), jnp.concatenate([low, low], axis=1)], axis=0
    )


def apply_rows(stacked, maps):
    out = lax.dot_general(
        stacked, maps, (((1,), (1,)), ((), ())), preferred_element_type=f32
    )
    half = out.shape[0] // 2
    return out[:half] + out[half:]


def rollout_kernel(
    n, nx, nu, tl, sl,
    a_hbm, k_hbm, ff_hbm, d_hbm, x0_hbm, x_tile, u_tile,
    a_ref, k_ref, ff_ref, d_ref, x0_ref,
    leaf, nodes, pre, wf, tile, x_send, x_all, t_send, t_recv, p_send, m_recv, e_send, e_recv, send, recv,
    in_sem, x_ssem, x_rsem, t_ssem, t_rsem, m_ssem, m_rsem, p_ssem, o_ssem, o_rsem,
):
    D = tile.shape[0]
    dr = t_send.shape[0]
    rows = nx + nu
    pairs = n // 2
    me = lax.axis_index("tm")
    pair, odd = me // 2, me % 2

    def load(src, dst, i):
        return pltpu.make_async_copy(src, dst, in_sem.at[i])

    a_load = load(a_hbm, a_ref, 4)
    d_load, x_load = load(d_hbm, d_ref, 0), load(x0_hbm, x0_ref, 1)
    f_load, k_load = load(ff_hbm, ff_ref, 2), load(k_hbm, k_ref, 3)
    for copy in (d_load, a_load, x_load, f_load):
        copy.start()
    barrier = pltpu.get_barrier_semaphore()
    for k in range(1, n):
        pl.semaphore_signal(
            barrier, inc=1, device_id={"tm": (me + k) % n}, device_id_type=MESH
        )

    lane = lax.broadcasted_iota(jnp.int32, (D, D), 1)
    row = lax.broadcasted_iota(jnp.int32, (D, D), 0)
    corner = jnp.where((lane == nx) & (row == nx), 1.0, 0.0).astype(f32)

    tile[...] = jnp.zeros((D, D), f32)
    d_load.wait()
    tile[0:tl, 0:nx] = d_ref[...]
    d_cols = jnp.transpose(tile[...])
    side = jnp.zeros((nx, D - nx), f32)
    side_u = jnp.zeros((nu, D - nx), f32)
    foot = jnp.zeros((D - nx, D), f32)

    def make_leaf(t):
        a = jnp.concatenate([jnp.concatenate([a_ref[t], side], axis=1), foot], axis=0)
        a = jnp.where(lane == nx, pltpu.roll(d_cols, nx - t, 1), a) + corner
        leaf[t, 0:D] = split(a)

    def node(level, k):
        if level == 0:
            return leaf[k, 0:D]
        return nodes[tl - 2 * (tl >> level) + k]

    levels = tl.bit_length() - 1
    batch = BATCH

    def climb(level, first, last):
        for start in range(first, last, batch):
            group = range(start, min(last, start + batch))
            values = [product(node(level - 1, 2 * k + 1), node(level - 1, 2 * k)) for k in group]
            if level == levels:
                return values[0]
            for k, value in zip(group, values):
                nodes[tl - 2 * (tl >> level) + k] = split(value)

    a_load.wait()
    k_load.start()
    for t in range(tl):
        make_leaf(t)
    root = climb(1, 0, tl // 2)

    def x_copy(src, k):
        return pltpu.make_async_remote_copy(
            src_ref=x_send, dst_ref=x_all.at[src],
            send_sem=x_ssem, recv_sem=x_rsem,
            device_id={"tm": 2 * ((pair + k) % pairs) + 1}, device_id_type=MESH,
        )

    def send_x():
        pl.semaphore_wait(barrier, n - 1)
        x_load.wait()
        x_rows = jnp.concatenate([x0_ref[...], jnp.zeros((sl, D - nx), f32)], axis=1)
        x_rows = jnp.where(lax.broadcasted_iota(jnp.int32, (sl, D), 1) == nx, 1.0, x_rows)
        x_send[...] = x_rows
        x_all[me] = x_rows
        for k in range(1, pairs):
            x_copy(me, k).start()

        @pl.when(odd == 0)
        def _():
            x_copy(me, 0).start()

    @pl.when(pair > 0)
    def _():
        send_x()

    for level in range(2, levels + 1):
        root = climb(level, 0, tl >> level)
    root_split = split(root)
    t_send[...] = root[:dr]

    @pl.when(pair == 0)
    def _():
        send_x()

    def x_wait(count):
        return pltpu.make_async_remote_copy(
            src_ref=x_all.at[pl.ds(0, count)], dst_ref=x_all.at[pl.ds(0, count)],
            send_sem=x_ssem, recv_sem=x_rsem, device_id={"tm": me}, device_id_type=MESH,
        )

    def to_partner(src, dst, ssem, rsem):
        return pltpu.make_async_remote_copy(
            src_ref=src, dst_ref=dst, send_sem=ssem, recv_sem=rsem,
            device_id={"tm": me + 1 - 2 * odd}, device_id_type=MESH,
        )

    t_copy = to_partner(t_send, t_recv, t_ssem, t_rsem)
    e_copy = to_partner(e_send, e_recv, p_ssem, m_rsem.at[0])
    def m_copy(src, slot, dst, ssem):
        return pltpu.make_async_remote_copy(
            src_ref=src, dst_ref=m_recv.at[slot], send_sem=ssem, recv_sem=m_rsem.at[slot],
            device_id={"tm": 2 * dst + 1}, device_id_type=MESH,
        )

    direct = jnp.where(pair == 0, pairs, pairs - 1)

    def go(j, c):
        q = direct + pair - j
        m_copy(t_send, me, q, m_ssem.at[q - 1]).start()
        return c

    lax.fori_loop(pair + 1, direct, go, 0)
    t_copy.start()

    f_load.wait()
    tile[...] = jnp.zeros((D, D), f32)
    tile[0:tl, 0:nu] = ff_ref[...]
    f_cols = jnp.transpose(tile[...])[:nu]
    lane_u = lax.broadcasted_iota(jnp.int32, (nu, D), 1)
    k_load.wait()

    def make_gain(t):
        g = -jnp.concatenate([k_ref[t], side_u], axis=1)
        g = jnp.where(lane_u == nx, pltpu.roll(f_cols, nx - t, 1), g)
        leaf[t, D : D + nu] = split(g)

    for t in range(tl):
        make_gain(t)

    eye = jnp.where((lane == row) & (lane <= nx), 1.0, 0.0).astype(f32)
    pre[0] = split(eye)
    wf[pl.ds(0, nx, stride=tl), :] = eye[:nx]

    def put_pre(t, value):
        pre[t] = split(value)
        wf[pl.ds(t, nx, stride=tl), :] = value[:nx]

    pad_rows = corner[dr:]

    def full(value):
        return split(jnp.concatenate([value, pad_rows], axis=0))

    passes = (odd == 0) & (pair > 0) & (pair + 1 < pairs)
    keeps = (odd == 0) & ((pair == 0) | (pair + 1 == pairs))
    p_copy = m_copy(p_send, pair + 1, pairs - 1, p_ssem)

    def pass_pair():
        @pl.when(passes)
        def _():
            t_copy.wait_recv()
            p_send[...] = product(full(t_recv[...]), root_split)[:dr]
            p_copy.start()

        @pl.when(keeps)
        def _():
            t_copy.wait_recv()

    for level in range(levels - 1, 0, -1):
        size = 1 << level
        put_first = nodes[tl - 2 * (tl >> level)]
        pre[size] = put_first
        wf[pl.ds(size, nx, stride=tl), :] = (
            put_first[:nx, :D].astype(f32) + put_first[:nx, D:].astype(f32)
        )
        count = (tl >> (level + 1)) - 1

        for first in range(0, count, batch):
            group = [2 * (j + 1) for j in range(first, min(count, first + batch))]
            values = [product(node(level, k), pre[size * k]) for k in group]
            for k, value in zip(group, values):
                put_pre(size * (k + 1), value)
        if level == min(2, levels - 1):
            pass_pair()

    for first in range(0, tl, 2 * WIDE):
        group = range(first, min(tl, first + 2 * WIDE), 2)
        values = [product(leaf[t], pre[t]) for t in group]
        for t, value in zip(group, values):
            put_pre(t + 1, value[:D])
            wf[pl.ds(nx * tl + t, nu, stride=tl), :] = value[D:]
        values = [product(leaf[t + 1, D : D + nu], pre[t + 1]) for t in group]
        for t, value in zip(group, values):
            wf[pl.ds(nx * tl + t + 1, nu, stride=tl), :] = value

    @pl.when(odd == 1)
    def _():
        x_wait(n - 1).wait_recv()
        entry = jnp.concatenate([x_all[k] for k in range(n)], axis=0)

        def chain(k, entry):
            m_copy(t_send, k, pair, p_ssem).wait_recv()
            return apply_rows(stack_rows(entry), full(m_recv[k]))

        count = jnp.where(pair == pairs - 1, min(pairs, 2 * pairs - 2), 2 * pair)
        entry = lax.fori_loop(0, count, chain, entry)
        e_send[...] = entry
        e_copy.start()
        t_copy.wait_recv()
        e_recv[...] = apply_rows(stack_rows(entry), full(t_recv[...]))

    @pl.when(odd == 0)
    def _():
        e_copy.wait_recv()

    entry = e_recv[...]
    stacked = stack_rows(entry)

    chunks = spans(rows * tl, 4 * LANES)
    group = LANES // tl

    def o_copy(src, dst, c):
        start, stop = chunks[c]
        part = pl.ds(start, stop - start)
        return pltpu.make_async_remote_copy(
            src_ref=send.at[dst, :, part], dst_ref=recv.at[src, :, part],
            send_sem=o_ssem, recv_sem=o_rsem.at[c, src // group],
            device_id={"tm": dst}, device_id_type=MESH,
        )

    def o_wait(count, start, stop, sem):
        part = (pl.ds(0, count), slice(None), pl.ds(start, stop - start))
        return pltpu.make_async_remote_copy(
            src_ref=send.at[part], dst_ref=recv.at[part], send_sem=o_ssem, recv_sem=sem,
            device_id={"tm": me}, device_id_type=MESH,
        )

    peers = order(me, n)
    for c, (start, stop) in enumerate(chunks):
        for first in range(start, stop, 4 * LANES):
            here = slice(first, first + 4 * LANES)
            part = apply_rows(stacked, split(wf[here, :]))
            for d in range(n):
                send[d, :, here] = part[d * sl : (d + 1) * sl]
        recv[me, :, start:stop] = send[me, :, start:stop]
        for dst in peers:
            o_copy(me, dst, c).start()

    t_copy.wait_send()

    @pl.when(odd == 0)
    def _():
        x_wait(pairs).wait_send()

    def done(q, c):
        m_copy(t_send, me, q, m_ssem.at[q - 1]).wait_send()
        return c

    lax.fori_loop(pair + 1, direct, done, 0)

    @pl.when(passes)
    def _():
        p_copy.wait_send()

    @pl.when(odd == 1)
    def _():
        x_wait(pairs - 1).wait_send()
        e_copy.wait_send()

    for c, (start, stop) in enumerate(chunks):
        for h in range(n // group):
            for count in (group - 1, group):
                @pl.when((me // group == h) == (count < group))
                def _(count=count, start=start, stop=stop, c=c, h=h):
                    o_wait(count, start, stop, o_rsem.at[c, h]).wait_recv()

            for q in range(start // LANES, stop // LANES):
                values = exchange(
                    [recv[h * group + b, :, q * LANES : (q + 1) * LANES] for b in range(group)], tl
                )
                for i, value in enumerate(values):
                    index = q * group + i
                    if index < nx:
                        x_tile[h, pl.ds(index, sl, stride=nx), :] = value
                    else:
                        u_tile[h, pl.ds(index - nx, sl, stride=nu), :] = value

    o_wait(n - 1, 0, rows * tl, o_rsem.at[0, 0]).wait_send()


def store_kernel(halves, x_ref, u_ref, states_hbm, controls_hbm, sem):
    copies = [
        pltpu.make_async_copy(
            src.at[h], dst.at[:, :, pl.ds(h * LANES, LANES)], sem.at[i, h]
        )
        for i, (src, dst) in enumerate(((x_ref, states_hbm), (u_ref, controls_hbm)))
        for h in range(halves)
    ]
    for copy in copies:
        copy.start()
    for copy in copies:
        copy.wait()


def body(closed_loop, gains, feedforward, drift_terms, initial_states):
    tl, nx = closed_loop.shape[:2]
    nu = gains.shape[1]
    sl = initial_states.shape[1]
    n = lax.axis_size("tm")
    D = up(nx + 1, LANES)
    dr = up(nx, 8)
    rows = nx + nu
    vmem = pl.BlockSpec(memory_space=pltpu.VMEM)
    dma = pltpu.SemaphoreType.DMA
    hbm = pl.BlockSpec(memory_space=pltpu.HBM)
    chunks = len(spans(rows * tl, 4 * LANES))
    steps = n * tl
    halves = steps // LANES
    x_tile, u_tile = pl.pallas_call(
        functools.partial(rollout_kernel, n, nx, nu, tl, sl),
        out_shape=(
            jax.ShapeDtypeStruct((halves, sl * nx, LANES), f32),
            jax.ShapeDtypeStruct((halves, sl * nu, LANES), f32),
        ),
        in_specs=[hbm] * 5,
        out_specs=(vmem, vmem),
        scratch_shapes=[
            pltpu.VMEM((tl, nx, nx), f32),
            pltpu.VMEM((tl, nu, nx), f32),
            pltpu.VMEM((tl, nu), f32),
            pltpu.VMEM((tl, nx), f32),
            pltpu.VMEM((sl, nx), f32),
            pltpu.VMEM((tl, D + nu, 2 * D), bf16),
            pltpu.VMEM((tl, D, 2 * D), bf16),
            pltpu.VMEM((tl, D, 2 * D), bf16),
            pltpu.VMEM((rows * tl, D), f32),
            pltpu.VMEM((D, D), f32),
            pltpu.VMEM((sl, D), f32),
            pltpu.VMEM((n, sl, D), f32),
            pltpu.VMEM((dr, D), f32),
            pltpu.VMEM((dr, D), f32),
            pltpu.VMEM((dr, D), f32),
            pltpu.VMEM((n, dr, D), f32),
            pltpu.VMEM((n * sl, D), f32),
            pltpu.VMEM((n * sl, D), f32),
            pltpu.VMEM((n, sl, rows * tl), f32),
            pltpu.VMEM((n, sl, rows * tl), f32),
            dma((5,)),
            dma, dma, dma, dma, dma((max(n // 2 - 1, 1),)), dma((max(n - 2, 1),)), dma,
            dma, dma((chunks, halves)),
        ],
        compiler_params=pltpu.CompilerParams(
            collective_id=0, has_side_effects=True, vmem_limit_bytes=48 * 2**20
        ),
    )(
        *(
            pltpu.with_memory_space_constraint(value, pltpu.HBM)
            for value in (closed_loop, gains, feedforward, drift_terms, initial_states.T)
        )
    )
    return pl.pallas_call(
        functools.partial(store_kernel, halves),
        out_shape=(
            jax.ShapeDtypeStruct((sl, nx, steps), f32),
            jax.ShapeDtypeStruct((sl, nu, steps), f32),
        ),
        in_specs=[vmem] * 2,
        out_specs=(hbm, hbm),
        scratch_shapes=[dma((2, halves))],
        compiler_params=pltpu.CompilerParams(vmem_limit_bytes=2**20),
    )(x_tile.reshape(halves, sl, nx, LANES), u_tile.reshape(halves, sl, nu, LANES))


def solution(mesh):
    return jax.shard_map(
        body,
        mesh=mesh,
        in_specs=(
            P("tm", None, None),
            P("tm", None, None),
            P("tm", None),
            P("tm", None),
            P(None, ("tm", "scen")),
        ),
        out_specs=(P(("tm", "scen"), None, None), P(("tm", "scen"), None, None)),
        check_vma=False,
    )
```

```python
import functools
import jax
import jax.numpy as jnp
from jax import lax
from jax.experimental import pallas as pl
from jax.experimental.pallas import tpu as pltpu
from jax.sharding import PartitionSpec as P

LANES = 128
SIZES = (2, 4)
BATCH = 4
WIDE = 8
MESH = pl.DeviceIdType.MESH
f32 = jnp.float32
bf16 = jnp.bfloat16


def spans(total, unit):
    left, edges = total // unit, [0]
    for size in SIZES:
        if size < left:
            left -= size
            edges.append(edges[-1] + size * unit)
    return list(zip(edges, edges[1:] + [total]))


def order(me, n):
    if n != 8:
        return [(me + k) % n for k in range(1, n)]
    rows = ((1, 0, 2, 3), (0, 1, 3, 2), (0, 2, 1, 3), (0, 3, 1, 2))
    table = [[2 * p + d if p != m // 2 else m + 1 - 2 * (m % 2) for p in rows[m // 2] for d in range(1 + (p != m // 2))] for m in range(n)]
    return [
        functools.reduce(lambda acc, m: jnp.where(me == m, table[m][k], acc), range(n), 0)
        for k in range(n - 1)
    ]


def exchange(values, tl):
    group = len(values)
    lane = lax.broadcasted_iota(jnp.int32, values[0].shape, 1) // tl
    gap = group // 2
    while gap:
        low = (lane // gap) % 2 == 0
        out = list(values)
        for i in range(group):
            if (i // gap) % 2 == 0:
                a, b = values[i], values[i + gap]
                out[i] = jnp.where(low, a, pltpu.roll(b, gap * tl, 1))
                out[i + gap] = jnp.where(low, pltpu.roll(a, LANES - gap * tl, 1), b)
        values = out
        gap //= 2
    return values


def up(value, unit):
    return -(-value // unit) * unit


def split(value):
    high = value.astype(bf16)
    low = (value - high.astype(f32)).astype(bf16)
    return jnp.concatenate([high, low], axis=1)


def product(left, right):
    wide = right.shape[1] // 2
    pad = jnp.zeros((wide - right.shape[0], 2 * wide), bf16)
    both = jnp.concatenate([right, pad, right, pad], axis=0)
    out = jnp.dot(left, both, preferred_element_type=f32)
    return out[:, :wide] + out[:, wide:]


def stack_rows(rows):
    high = rows.astype(bf16)
    low = (rows - high.astype(f32)).astype(bf16)
    return jnp.concatenate(
        [jnp.concatenate([high, high], axis=1), jnp.concatenate([low, low], axis=1)], axis=0
    )


def apply_rows(stacked, maps):
    out = lax.dot_general(
        stacked, maps, (((1,), (1,)), ((), ())), preferred_element_type=f32
    )
    half = out.shape[0] // 2
    return out[:half] + out[half:]


def advance(rows, maps):
    wide = maps.shape[1] // 2
    high, low = maps[:, :wide], maps[:, wide:]
    both = jnp.concatenate(
        [jnp.concatenate([high, high], axis=1), jnp.concatenate([low, low], axis=1)], axis=0
    )
    out = lax.dot_general(
        split(rows), both, (((1,), (1,)), ((), ())), preferred_element_type=f32
    )
    return out[:, :wide] + out[:, wide:]


def rollout_kernel(
    n, nx, nu, tl, sl,
    a_hbm, k_hbm, ff_hbm, d_hbm, x0_hbm, x_tile, u_tile,
    a_ref, k_ref, ff_ref, d_ref, x0_ref,
    leaf, nodes, pre, wf, tile, x_send, x_all, t_send, t_recv, p_send, m_recv, e_send, e_recv, send, recv,
    in_sem, x_ssem, x_rsem, t_ssem, t_rsem, m_ssem, m_rsem, p_ssem, o_ssem, o_rsem,
):
    D = tile.shape[0]
    R = pre.shape[1]
    dr = t_send.shape[0]
    rows = nx + nu
    pairs = n // 2
    me = lax.axis_index("tm")
    pair, odd = me // 2, me % 2

    def load(src, dst, i):
        return pltpu.make_async_copy(src, dst, in_sem.at[i])

    a_load = load(a_hbm, a_ref, 4)
    d_load, x_load = load(d_hbm, d_ref, 0), load(x0_hbm, x0_ref, 1)
    f_load, k_load = load(ff_hbm, ff_ref, 2), load(k_hbm, k_ref, 3)
    for copy in (d_load, a_load, x_load, f_load):
        copy.start()
    barrier = pltpu.get_barrier_semaphore()
    for k in range(1, n):
        pl.semaphore_signal(
            barrier, inc=1, device_id={"tm": (me + k) % n}, device_id_type=MESH
        )

    lane = lax.broadcasted_iota(jnp.int32, (D, D), 1)
    row = lax.broadcasted_iota(jnp.int32, (D, D), 0)
    corner = jnp.where((lane == nx) & (row == nx), 1.0, 0.0).astype(f32)

    tile[...] = jnp.zeros((D, D), f32)
    d_load.wait()
    tile[0:tl, 0:nx] = d_ref[...]
    d_cols = jnp.transpose(tile[...])[:nx]
    side = jnp.zeros((nx, D - nx), f32)
    side_u = jnp.zeros((nu, D - nx), f32)
    foot = split(corner[nx:R])
    lane_x = lax.broadcasted_iota(jnp.int32, (nx, D), 1)

    def make_leaf(t):
        a = jnp.concatenate([a_ref[t], side], axis=1)
        leaf[t, 0:nx] = split(jnp.where(lane_x == nx, pltpu.roll(d_cols, nx - t, 1), a))
        leaf[t, nx:R] = foot

    def node(level, k):
        if level == 0:
            return leaf[k, 0:R]
        return nodes[tl - 2 * (tl >> level) + k]

    levels = tl.bit_length() - 1
    batch = BATCH

    def climb(level, first, last):
        for start in range(first, last, batch):
            group = range(start, min(last, start + batch))
            values = [product(node(level - 1, 2 * k + 1), node(level - 1, 2 * k)) for k in group]
            if level == levels:
                return values[0]
            for k, value in zip(group, values):
                nodes[tl - 2 * (tl >> level) + k] = split(value)

    a_load.wait()
    k_load.start()
    for t in range(tl):
        make_leaf(t)
    root = climb(1, 0, tl // 2)

    def x_copy(src, k):
        return pltpu.make_async_remote_copy(
            src_ref=x_send, dst_ref=x_all.at[src],
            send_sem=x_ssem, recv_sem=x_rsem,
            device_id={"tm": 2 * ((pair + k) % pairs) + 1}, device_id_type=MESH,
        )

    def send_x():
        pl.semaphore_wait(barrier, n - 1)
        x_load.wait()
        x_rows = jnp.concatenate([x0_ref[...], jnp.zeros((sl, D - nx), f32)], axis=1)
        x_rows = jnp.where(lax.broadcasted_iota(jnp.int32, (sl, D), 1) == nx, 1.0, x_rows)
        x_send[...] = x_rows
        x_all[me] = x_rows
        for k in range(1, pairs):
            x_copy(me, k).start()

        @pl.when(odd == 0)
        def _():
            x_copy(me, 0).start()

    @pl.when(pair > 0)
    def _():
        send_x()

    for level in range(2, levels + 1):
        root = climb(level, 0, tl >> level)
    root_split = split(root)
    t_send[...] = root[:dr]

    @pl.when(pair == 0)
    def _():
        send_x()

    def x_wait(count):
        return pltpu.make_async_remote_copy(
            src_ref=x_all.at[pl.ds(0, count)], dst_ref=x_all.at[pl.ds(0, count)],
            send_sem=x_ssem, recv_sem=x_rsem, device_id={"tm": me}, device_id_type=MESH,
        )

    def to_partner(src, dst, ssem, rsem):
        return pltpu.make_async_remote_copy(
            src_ref=src, dst_ref=dst, send_sem=ssem, recv_sem=rsem,
            device_id={"tm": me + 1 - 2 * odd}, device_id_type=MESH,
        )

    t_copy = to_partner(t_send, t_recv, t_ssem, t_rsem)
    e_copy = to_partner(e_send, e_recv, p_ssem, m_rsem.at[0])
    def m_copy(src, slot, dst, ssem):
        return pltpu.make_async_remote_copy(
            src_ref=src, dst_ref=m_recv.at[slot], send_sem=ssem, recv_sem=m_rsem.at[slot],
            device_id={"tm": 2 * dst + 1}, device_id_type=MESH,
        )

    direct = jnp.where(pair == 0, pairs, pairs - 1)

    def go(j, c):
        q = direct + pair - j
        m_copy(t_send, me, q, m_ssem.at[q - 1]).start()
        return c

    lax.fori_loop(pair + 1, direct, go, 0)
    t_copy.start()

    eye = jnp.where((lane == row) & (lane <= nx), 1.0, 0.0).astype(f32)
    pre[0] = split(eye[:R])
    wf[pl.ds(0, nx, stride=tl), :] = eye[:nx]

    def put_pre(t, value):
        pre[t] = split(value)
        wf[pl.ds(t, nx, stride=tl), :] = value[:nx]

    pad_rows = corner[dr:]

    def full(value):
        return split(jnp.concatenate([value, pad_rows], axis=0))

    passes = (odd == 0) & (pair > 0) & (pair + 1 < pairs)
    keeps = (odd == 0) & ((pair == 0) | (pair + 1 == pairs))
    p_copy = m_copy(p_send, pair + 1, pairs - 1, p_ssem)

    def pass_pair():
        @pl.when(passes)
        def _():
            t_copy.wait_recv()
            p_send[...] = product(split(t_recv[...]), root_split)
            p_copy.start()

        @pl.when(keeps)
        def _():
            t_copy.wait_recv()

    for level in range(levels - 1, 0, -1):
        size = 1 << level
        put_first = nodes[tl - 2 * (tl >> level)]
        pre[size] = put_first
        wf[pl.ds(size, nx, stride=tl), :] = (
            put_first[:nx, :D].astype(f32) + put_first[:nx, D:].astype(f32)
        )
        count = (tl >> (level + 1)) - 1

        for first in range(0, count, batch):
            group = [2 * (j + 1) for j in range(first, min(count, first + batch))]
            values = [product(node(level, k), pre[size * k]) for k in group]
            for k, value in zip(group, values):
                put_pre(size * (k + 1), value)
        if level == min(2, levels - 1):
            pass_pair()

    for first in range(0, tl, 2 * WIDE):
        group = range(first, min(tl, first + 2 * WIDE), 2)
        values = [product(leaf[t, 0:R], pre[t]) for t in group]
        for t, value in zip(group, values):
            put_pre(t + 1, value)

    def make_controls():
        f_load.wait()
        tile[...] = jnp.zeros((D, D), f32)
        tile[0:tl, 0:nu] = ff_ref[...]
        f_cols = jnp.transpose(tile[...])[:nu]
        lane_u = lax.broadcasted_iota(jnp.int32, (nu, D), 1)
        k_load.wait()

        def make_gain(t):
            g = -jnp.concatenate([k_ref[t], side_u], axis=1)
            g = jnp.where(lane_u == nx, pltpu.roll(f_cols, nx - t, 1), g)
            leaf[t, R : R + nu] = split(g)

        for t in range(tl):
            make_gain(t)


        for first in range(0, tl, WIDE):
            group = range(first, min(tl, first + WIDE))
            values = [product(leaf[t, R : R + nu], pre[t]) for t in group]
            for t, value in zip(group, values):
                wf[pl.ds(nx * tl + t, nu, stride=tl), :] = value

    @pl.when(odd == 1)
    def _():
        x_wait(n - 1).wait_recv()
        entry = jnp.concatenate([x_all[k] for k in range(n)], axis=0)

        def chain(k, entry):
            m_copy(t_send, k, pair, p_ssem).wait_recv()
            return advance(entry, full(m_recv[k]))

        count = jnp.where(pair == pairs - 1, min(pairs, 2 * pairs - 2), 2 * pair)
        entry = lax.fori_loop(0, count, chain, entry)
        e_send[...] = entry
        e_copy.start()
        t_copy.wait_recv()
        e_recv[...] = advance(entry, full(t_recv[...]))

    @pl.when(odd == 0)
    def _():
        make_controls()
        e_copy.wait_recv()

    entry = e_recv[...]
    stacked = stack_rows(entry)

    chunks = spans(rows * tl, 4 * LANES)
    group = LANES // tl

    def o_copy(src, dst, c):
        start, stop = chunks[c]
        part = pl.ds(start, stop - start)
        return pltpu.make_async_remote_copy(
            src_ref=send.at[dst, :, part], dst_ref=recv.at[src, :, part],
            send_sem=o_ssem, recv_sem=o_rsem.at[c, src // group],
            device_id={"tm": dst}, device_id_type=MESH,
        )

    def o_wait(count, start, stop, sem):
        part = (pl.ds(0, count), slice(None), pl.ds(start, stop - start))
        return pltpu.make_async_remote_copy(
            src_ref=send.at[part], dst_ref=recv.at[part], send_sem=o_ssem, recv_sem=sem,
            device_id={"tm": me}, device_id_type=MESH,
        )

    peers = order(me, n)
    mixed = min(c for c, (_, stop) in enumerate(chunks) if stop > nx * tl)
    for c, (start, stop) in enumerate(chunks):
        if c == mixed:

            @pl.when(odd == 1)
            def _():
                make_controls()

        for first in range(start, stop, 4 * LANES):
            here = slice(first, first + 4 * LANES)
            part = apply_rows(stacked, split(wf[here, :]))
            for d in range(n):
                send[d, :, here] = part[d * sl : (d + 1) * sl]
        recv[me, :, start:stop] = send[me, :, start:stop]
        for dst in peers:
            o_copy(me, dst, c).start()

    t_copy.wait_send()

    @pl.when(odd == 0)
    def _():
        x_wait(pairs).wait_send()

    def done(q, c):
        m_copy(t_send, me, q, m_ssem.at[q - 1]).wait_send()
        return c

    lax.fori_loop(pair + 1, direct, done, 0)

    @pl.when(passes)
    def _():
        p_copy.wait_send()

    @pl.when(odd == 1)
    def _():
        x_wait(pairs - 1).wait_send()
        e_copy.wait_send()

    for c, (start, stop) in enumerate(chunks):
        for h in range(n // group):
            for count in (group - 1, group):
                @pl.when((me // group == h) == (count < group))
                def _(count=count, start=start, stop=stop, c=c, h=h):
                    o_wait(count, start, stop, o_rsem.at[c, h]).wait_recv()

            for q in range(start // LANES, stop // LANES):
                values = exchange(
                    [recv[h * group + b, :, q * LANES : (q + 1) * LANES] for b in range(group)], tl
                )
                for i, value in enumerate(values):
                    index = q * group + i
                    if index < nx:
                        x_tile[h, pl.ds(index, sl, stride=nx), :] = value
                    else:
                        u_tile[h, pl.ds(index - nx, sl, stride=nu), :] = value

    o_wait(n - 1, 0, rows * tl, o_rsem.at[0, 0]).wait_send()


def store_kernel(halves, x_ref, u_ref, states_hbm, controls_hbm, sem):
    copies = [
        pltpu.make_async_copy(
            src.at[h], dst.at[:, :, pl.ds(h * LANES, LANES)], sem.at[i, h]
        )
        for i, (src, dst) in enumerate(((x_ref, states_hbm), (u_ref, controls_hbm)))
        for h in range(halves)
    ]
    for copy in copies:
        copy.start()
    for copy in copies:
        copy.wait()


def body(closed_loop, gains, feedforward, drift_terms, initial_states):
    tl, nx = closed_loop.shape[:2]
    nu = gains.shape[1]
    sl = initial_states.shape[1]
    n = lax.axis_size("tm")
    D = up(nx + 1, LANES)
    dr = up(nx, 8)
    R = up(nx + 1, 16)
    rows = nx + nu
    vmem = pl.BlockSpec(memory_space=pltpu.VMEM)
    dma = pltpu.SemaphoreType.DMA
    hbm = pl.BlockSpec(memory_space=pltpu.HBM)
    chunks = len(spans(rows * tl, 4 * LANES))
    steps = n * tl
    halves = steps // LANES
    x_tile, u_tile = pl.pallas_call(
        functools.partial(rollout_kernel, n, nx, nu, tl, sl),
        out_shape=(
            jax.ShapeDtypeStruct((halves, sl * nx, LANES), f32),
            jax.ShapeDtypeStruct((halves, sl * nu, LANES), f32),
        ),
        in_specs=[hbm] * 5,
        out_specs=(vmem, vmem),
        scratch_shapes=[
            pltpu.VMEM((tl, nx, nx), f32),
            pltpu.VMEM((tl, nu, nx), f32),
            pltpu.VMEM((tl, nu), f32),
            pltpu.VMEM((tl, nx), f32),
            pltpu.VMEM((sl, nx), f32),
            pltpu.VMEM((tl, R + nu, 2 * D), bf16),
            pltpu.VMEM((tl, R, 2 * D), bf16),
            pltpu.VMEM((tl, R, 2 * D), bf16),
            pltpu.VMEM((rows * tl, D), f32),
            pltpu.VMEM((D, D), f32),
            pltpu.VMEM((sl, D), f32),
            pltpu.VMEM((n, sl, D), f32),
            pltpu.VMEM((dr, D), f32),
            pltpu.VMEM((dr, D), f32),
            pltpu.VMEM((dr, D), f32),
            pltpu.VMEM((n, dr, D), f32),
            pltpu.VMEM((n * sl, D), f32),
            pltpu.VMEM((n * sl, D), f32),
            pltpu.VMEM((n, sl, rows * tl), f32),
            pltpu.VMEM((n, sl, rows * tl), f32),
            dma((5,)),
            dma, dma, dma, dma, dma((max(n // 2 - 1, 1),)), dma((max(n - 2, 1),)), dma,
            dma, dma((chunks, halves)),
        ],
        compiler_params=pltpu.CompilerParams(
            collective_id=0, has_side_effects=True, vmem_limit_bytes=48 * 2**20
        ),
    )(
        *(
            pltpu.with_memory_space_constraint(value, pltpu.HBM)
            for value in (closed_loop, gains, feedforward, drift_terms, initial_states.T)
        )
    )
    return pl.pallas_call(
        functools.partial(store_kernel, halves),
        out_shape=(
            jax.ShapeDtypeStruct((sl, nx, steps), f32),
            jax.ShapeDtypeStruct((sl, nu, steps), f32),
        ),
        in_specs=[vmem] * 2,
        out_specs=(hbm, hbm),
        scratch_shapes=[dma((2, halves))],
        compiler_params=pltpu.CompilerParams(vmem_limit_bytes=2**20),
    )(x_tile.reshape(halves, sl, nx, LANES), u_tile.reshape(halves, sl, nu, LANES))


def solution(mesh):
    return jax.shard_map(
        body,
        mesh=mesh,
        in_specs=(
            P("tm", None, None),
            P("tm", None, None),
            P("tm", None),
            P("tm", None),
            P(None, ("tm", "scen")),
        ),
        out_specs=(P(("tm", "scen"), None, None), P(("tm", "scen"), None, None)),
        check_vma=False,
    )
```

```python
import functools
import jax
import jax.numpy as jnp
from jax import lax
from jax.experimental import pallas as pl
from jax.experimental.pallas import tpu as pltpu
from jax.sharding import PartitionSpec as P

LANES = 128
SIZES = (1, 2, 3)
BATCH = 4
WIDE = 8
MESH = pl.DeviceIdType.MESH
f32 = jnp.float32
bf16 = jnp.bfloat16


def spans(total, unit):
    left, edges = total // unit, [0]
    for size in SIZES:
        if size < left:
            left -= size
            edges.append(edges[-1] + size * unit)
    return list(zip(edges, edges[1:] + [total]))


def order(me, n):
    if n != 8:
        return [(me + k) % n for k in range(1, n)]
    rows = ((1, 0, 2, 3), (0, 1, 3, 2), (0, 2, 1, 3), (0, 3, 1, 2))
    table = [[2 * p + d if p != m // 2 else m + 1 - 2 * (m % 2) for p in rows[m // 2] for d in range(1 + (p != m // 2))] for m in range(n)]
    return [
        functools.reduce(lambda acc, m: jnp.where(me == m, table[m][k], acc), range(n), 0)
        for k in range(n - 1)
    ]


def exchange(values, tl):
    group = len(values)
    lane = lax.broadcasted_iota(jnp.int32, values[0].shape, 1) // tl
    gap = group // 2
    while gap:
        low = (lane // gap) % 2 == 0
        out = list(values)
        for i in range(group):
            if (i // gap) % 2 == 0:
                a, b = values[i], values[i + gap]
                out[i] = jnp.where(low, a, pltpu.roll(b, gap * tl, 1))
                out[i + gap] = jnp.where(low, pltpu.roll(a, LANES - gap * tl, 1), b)
        values = out
        gap //= 2
    return values


def up(value, unit):
    return -(-value // unit) * unit


def split(value):
    high = value.astype(bf16)
    low = (value - high.astype(f32)).astype(bf16)
    return jnp.concatenate([high, low], axis=1)


def product(left, right):
    wide = right.shape[1] // 2
    pad = jnp.zeros((wide - right.shape[0], 2 * wide), bf16)
    both = jnp.concatenate([right, pad, right, pad], axis=0)
    out = jnp.dot(left, both, preferred_element_type=f32)
    return out[:, :wide] + out[:, wide:]


def stack_rows(rows):
    high = rows.astype(bf16)
    low = (rows - high.astype(f32)).astype(bf16)
    return jnp.concatenate(
        [jnp.concatenate([high, high], axis=1), jnp.concatenate([low, low], axis=1)], axis=0
    )


def apply_rows(stacked, maps):
    out = lax.dot_general(
        stacked, maps, (((1,), (1,)), ((), ())), preferred_element_type=f32
    )
    half = out.shape[0] // 2
    return out[:half] + out[half:]


def advance(rows, maps):
    wide = maps.shape[1] // 2
    high, low = maps[:, :wide], maps[:, wide:]
    both = jnp.concatenate(
        [jnp.concatenate([high, high], axis=1), jnp.concatenate([low, low], axis=1)], axis=0
    )
    out = lax.dot_general(
        split(rows), both, (((1,), (1,)), ((), ())), preferred_element_type=f32
    )
    return out[:, :wide] + out[:, wide:]


def rollout_kernel(
    n, nx, nu, tl, sl,
    a_hbm, k_hbm, ff_hbm, d_hbm, x0_hbm, x_tile, u_tile,
    a_ref, k_ref, ff_ref, d_ref, x0_ref,
    leaf, nodes, pre, wf, w2, tile, x_send, x_all, t_send, t_recv, p_send, m_recv, e_send, e_recv, send, recv,
    in_sem, x_ssem, x_rsem, t_ssem, t_rsem, m_ssem, m_rsem, p_ssem, o_ssem, o_rsem,
):
    D = tile.shape[0]
    R = pre.shape[1]
    dr = t_send.shape[0]
    rows = nx + nu
    pairs = n // 2
    me = lax.axis_index("tm")
    pair, odd = me // 2, me % 2

    def load(src, dst, i):
        return pltpu.make_async_copy(src, dst, in_sem.at[i])

    a_load = load(a_hbm, a_ref, 4)
    d_load, x_load = load(d_hbm, d_ref, 0), load(x0_hbm, x0_ref, 1)
    f_load, k_load = load(ff_hbm, ff_ref, 2), load(k_hbm, k_ref, 3)
    for copy in (d_load, a_load, x_load, f_load):
        copy.start()
    barrier = pltpu.get_barrier_semaphore()
    for k in range(1, n):
        pl.semaphore_signal(
            barrier, inc=1, device_id={"tm": (me + k) % n}, device_id_type=MESH
        )

    lane = lax.broadcasted_iota(jnp.int32, (D, D), 1)
    row = lax.broadcasted_iota(jnp.int32, (D, D), 0)
    corner = jnp.where((lane == nx) & (row == nx), 1.0, 0.0).astype(f32)

    tile[...] = jnp.zeros((D, D), f32)
    d_load.wait()
    tile[0:tl, 0:nx] = d_ref[...]
    d_cols = jnp.transpose(tile[...])[:nx]
    side = jnp.zeros((nx, D - nx), f32)
    side_u = jnp.zeros((nu, D - nx), f32)
    foot = split(corner[nx:R])
    lane_x = lax.broadcasted_iota(jnp.int32, (nx, D), 1)

    def make_leaf(t):
        a = jnp.concatenate([a_ref[t], side], axis=1)
        leaf[t, 0:nx] = split(jnp.where(lane_x == nx, pltpu.roll(d_cols, nx - t, 1), a))
        leaf[t, nx:R] = foot

    def node(level, k):
        if level == 0:
            return leaf[k, 0:R]
        return nodes[tl - 2 * (tl >> level) + k]

    levels = tl.bit_length() - 1
    batch = BATCH

    def climb(level, first, last):
        for start in range(first, last, batch):
            group = range(start, min(last, start + batch))
            values = [product(node(level - 1, 2 * k + 1), node(level - 1, 2 * k)) for k in group]
            if level == levels:
                return values[0]
            for k, value in zip(group, values):
                nodes[tl - 2 * (tl >> level) + k] = split(value)

    a_load.wait()
    k_load.start()
    for t in range(tl):
        make_leaf(t)
    root = climb(1, 0, tl // 2)

    def x_copy(src, k):
        return pltpu.make_async_remote_copy(
            src_ref=x_send, dst_ref=x_all.at[src],
            send_sem=x_ssem, recv_sem=x_rsem,
            device_id={"tm": 2 * ((pair + k) % pairs) + 1}, device_id_type=MESH,
        )

    def send_x():
        pl.semaphore_wait(barrier, n - 1)
        x_load.wait()
        x_rows = jnp.concatenate([x0_ref[...], jnp.zeros((sl, D - nx), f32)], axis=1)
        x_rows = jnp.where(lax.broadcasted_iota(jnp.int32, (sl, D), 1) == nx, 1.0, x_rows)
        x_send[...] = x_rows
        x_all[me] = x_rows
        for k in range(1, pairs):
            x_copy(me, k).start()

        @pl.when(odd == 0)
        def _():
            x_copy(me, 0).start()

    @pl.when(pair > 0)
    def _():
        send_x()

    for level in range(2, levels + 1):
        root = climb(level, 0, tl >> level)
    root_split = split(root)
    t_send[...] = root[:dr]

    @pl.when(pair == 0)
    def _():
        send_x()

    def x_wait(count):
        return pltpu.make_async_remote_copy(
            src_ref=x_all.at[pl.ds(0, count)], dst_ref=x_all.at[pl.ds(0, count)],
            send_sem=x_ssem, recv_sem=x_rsem, device_id={"tm": me}, device_id_type=MESH,
        )

    def to_partner(src, dst, ssem, rsem):
        return pltpu.make_async_remote_copy(
            src_ref=src, dst_ref=dst, send_sem=ssem, recv_sem=rsem,
            device_id={"tm": me + 1 - 2 * odd}, device_id_type=MESH,
        )

    t_copy = to_partner(t_send, t_recv, t_ssem, t_rsem)
    e_copy = to_partner(e_send, e_recv, p_ssem, m_rsem.at[0])
    def m_copy(src, slot, dst, ssem):
        return pltpu.make_async_remote_copy(
            src_ref=src, dst_ref=m_recv.at[slot], send_sem=ssem, recv_sem=m_rsem.at[slot],
            device_id={"tm": 2 * dst + 1}, device_id_type=MESH,
        )

    direct = jnp.where(pair == 0, pairs, pairs - 1)

    def go(j, c):
        q = direct + pair - j
        m_copy(t_send, me, q, m_ssem.at[q - 1]).start()
        return c

    lax.fori_loop(pair + 1, direct, go, 0)
    t_copy.start()

    eye = jnp.where((lane == row) & (lane <= nx), 1.0, 0.0).astype(f32)
    pre[0] = split(eye[:R])
    wf[pl.ds(0, nx, stride=tl), :] = eye[:nx]

    def put_pre(t, value):
        pre[t] = split(value)
        wf[pl.ds(t, nx, stride=tl), :] = value[:nx]

    pad_rows = corner[dr:]

    def full(value):
        return split(jnp.concatenate([value, pad_rows], axis=0))

    passes = (odd == 0) & (pair > 0) & (pair + 1 < pairs)
    keeps = (odd == 0) & ((pair == 0) | (pair + 1 == pairs))
    p_copy = m_copy(p_send, pair + 1, pairs - 1, p_ssem)

    def pass_pair():
        @pl.when(passes)
        def _():
            t_copy.wait_recv()
            p_send[...] = product(split(t_recv[...]), root_split)
            p_copy.start()

        @pl.when(keeps)
        def _():
            t_copy.wait_recv()

    for level in range(levels - 1, 0, -1):
        size = 1 << level
        put_first = nodes[tl - 2 * (tl >> level)]
        pre[size] = put_first
        wf[pl.ds(size, nx, stride=tl), :] = (
            put_first[:nx, :D].astype(f32) + put_first[:nx, D:].astype(f32)
        )
        count = (tl >> (level + 1)) - 1

        for first in range(0, count, batch):
            group = [2 * (j + 1) for j in range(first, min(count, first + batch))]
            values = [product(node(level, k), pre[size * k]) for k in group]
            for k, value in zip(group, values):
                put_pre(size * (k + 1), value)
        if level == min(2, levels - 1):
            pass_pair()

    for first in range(0, tl, 2 * WIDE):
        group = range(first, min(tl, first + 2 * WIDE), 2)
        values = [product(leaf[t, 0:R], pre[t]) for t in group]
        for t, value in zip(group, values):
            put_pre(t + 1, value)

    def make_controls():
        f_load.wait()
        tile[...] = jnp.zeros((D, D), f32)
        tile[0:tl, 0:nu] = ff_ref[...]
        f_cols = jnp.transpose(tile[...])[:nu]
        lane_u = lax.broadcasted_iota(jnp.int32, (nu, D), 1)
        k_load.wait()

        def make_gain(t):
            g = -jnp.concatenate([k_ref[t], side_u], axis=1)
            g = jnp.where(lane_u == nx, pltpu.roll(f_cols, nx - t, 1), g)
            leaf[t, R : R + nu] = split(g)

        for t in range(tl):
            make_gain(t)


        for first in range(0, tl, WIDE):
            group = range(first, min(tl, first + WIDE))
            values = [product(leaf[t, R : R + nu], pre[t]) for t in group]
            for t, value in zip(group, values):
                wf[pl.ds(nx * tl + t, nu, stride=tl), :] = value

    unit = 4 * LANES
    ready = nx * tl // unit * unit

    def halve(j, c):
        part = pl.ds(pl.multiple_of(j * unit, unit), unit)
        w2[part, :] = split(wf[part, :])
        return c

    lax.fori_loop(0, ready // unit, halve, 0)

    @pl.when(odd == 1)
    def _():
        x_wait(n - 1).wait_recv()
        entry = jnp.concatenate([x_all[k] for k in range(n)], axis=0)

        def chain(k, entry):
            m_copy(t_send, k, pair, p_ssem).wait_recv()
            return advance(entry, full(m_recv[k]))

        count = jnp.where(pair == pairs - 1, min(pairs, 2 * pairs - 2), 2 * pair)
        entry = lax.fori_loop(0, count, chain, entry)
        e_send[...] = entry
        e_copy.start()
        t_copy.wait_recv()
        e_recv[...] = advance(entry, full(t_recv[...]))

    @pl.when(odd == 0)
    def _():
        make_controls()
        e_copy.wait_recv()

    entry = e_recv[...]
    stacked = stack_rows(entry)

    chunks = spans(rows * tl, 4 * LANES)
    group = LANES // tl

    def o_copy(src, dst, c):
        start, stop = chunks[c]
        part = pl.ds(start, stop - start)
        return pltpu.make_async_remote_copy(
            src_ref=send.at[dst, :, part], dst_ref=recv.at[src, :, part],
            send_sem=o_ssem, recv_sem=o_rsem.at[c, src // group],
            device_id={"tm": dst}, device_id_type=MESH,
        )

    def o_wait(count, start, stop, sem):
        part = (pl.ds(0, count), slice(None), pl.ds(start, stop - start))
        return pltpu.make_async_remote_copy(
            src_ref=send.at[part], dst_ref=recv.at[part], send_sem=o_ssem, recv_sem=sem,
            device_id={"tm": me}, device_id_type=MESH,
        )

    peers = order(me, n)
    mixed = min(c for c, (_, stop) in enumerate(chunks) if stop > nx * tl)
    for c, (start, stop) in enumerate(chunks):
        if c == mixed:

            @pl.when(odd == 1)
            def _():
                make_controls()

        for first in range(start, stop, 4 * LANES):
            here = slice(first, first + 4 * LANES)
            part = apply_rows(stacked, w2[here, :] if first < ready else split(wf[here, :]))
            for d in range(n):
                send[d, :, here] = part[d * sl : (d + 1) * sl]
        recv[me, :, start:stop] = send[me, :, start:stop]
        for dst in peers:
            o_copy(me, dst, c).start()

    t_copy.wait_send()

    @pl.when(odd == 0)
    def _():
        x_wait(pairs).wait_send()

    def done(q, c):
        m_copy(t_send, me, q, m_ssem.at[q - 1]).wait_send()
        return c

    lax.fori_loop(pair + 1, direct, done, 0)

    @pl.when(passes)
    def _():
        p_copy.wait_send()

    @pl.when(odd == 1)
    def _():
        x_wait(pairs - 1).wait_send()
        e_copy.wait_send()

    for c, (start, stop) in enumerate(chunks):
        for h in range(n // group):
            for count in (group - 1, group):
                @pl.when((me // group == h) == (count < group))
                def _(count=count, start=start, stop=stop, c=c, h=h):
                    o_wait(count, start, stop, o_rsem.at[c, h]).wait_recv()

            for q in range(start // LANES, stop // LANES):
                values = exchange(
                    [recv[h * group + b, :, q * LANES : (q + 1) * LANES] for b in range(group)], tl
                )
                for i, value in enumerate(values):
                    index = q * group + i
                    if index < nx:
                        x_tile[h, pl.ds(index, sl, stride=nx), :] = value
                    else:
                        u_tile[h, pl.ds(index - nx, sl, stride=nu), :] = value

    o_wait(n - 1, 0, rows * tl, o_rsem.at[0, 0]).wait_send()


def store_kernel(halves, x_ref, u_ref, states_hbm, controls_hbm, sem):
    copies = [
        pltpu.make_async_copy(
            src.at[h], dst.at[:, :, pl.ds(h * LANES, LANES)], sem.at[i, h]
        )
        for i, (src, dst) in enumerate(((x_ref, states_hbm), (u_ref, controls_hbm)))
        for h in range(halves)
    ]
    for copy in copies:
        copy.start()
    for copy in copies:
        copy.wait()


def body(closed_loop, gains, feedforward, drift_terms, initial_states):
    tl, nx = closed_loop.shape[:2]
    nu = gains.shape[1]
    sl = initial_states.shape[1]
    n = lax.axis_size("tm")
    D = up(nx + 1, LANES)
    dr = up(nx, 8)
    R = up(nx + 1, 16)
    rows = nx + nu
    vmem = pl.BlockSpec(memory_space=pltpu.VMEM)
    dma = pltpu.SemaphoreType.DMA
    hbm = pl.BlockSpec(memory_space=pltpu.HBM)
    chunks = len(spans(rows * tl, 4 * LANES))
    steps = n * tl
    halves = steps // LANES
    x_tile, u_tile = pl.pallas_call(
        functools.partial(rollout_kernel, n, nx, nu, tl, sl),
        out_shape=(
            jax.ShapeDtypeStruct((halves, sl * nx, LANES), f32),
            jax.ShapeDtypeStruct((halves, sl * nu, LANES), f32),
        ),
        in_specs=[hbm] * 5,
        out_specs=(vmem, vmem),
        scratch_shapes=[
            pltpu.VMEM((tl, nx, nx), f32),
            pltpu.VMEM((tl, nu, nx), f32),
            pltpu.VMEM((tl, nu), f32),
            pltpu.VMEM((tl, nx), f32),
            pltpu.VMEM((sl, nx), f32),
            pltpu.VMEM((tl, R + nu, 2 * D), bf16),
            pltpu.VMEM((tl, R, 2 * D), bf16),
            pltpu.VMEM((tl, R, 2 * D), bf16),
            pltpu.VMEM((rows * tl, D), f32),
            pltpu.VMEM((rows * tl, 2 * D), bf16),
            pltpu.VMEM((D, D), f32),
            pltpu.VMEM((sl, D), f32),
            pltpu.VMEM((n, sl, D), f32),
            pltpu.VMEM((dr, D), f32),
            pltpu.VMEM((dr, D), f32),
            pltpu.VMEM((dr, D), f32),
            pltpu.VMEM((n, dr, D), f32),
            pltpu.VMEM((n * sl, D), f32),
            pltpu.VMEM((n * sl, D), f32),
            pltpu.VMEM((n, sl, rows * tl), f32),
            pltpu.VMEM((n, sl, rows * tl), f32),
            dma((5,)),
            dma, dma, dma, dma, dma((max(n // 2 - 1, 1),)), dma((max(n - 2, 1),)), dma,
            dma, dma((chunks, halves)),
        ],
        compiler_params=pltpu.CompilerParams(
            collective_id=0, has_side_effects=True, vmem_limit_bytes=48 * 2**20
        ),
    )(
        *(
            pltpu.with_memory_space_constraint(value, pltpu.HBM)
            for value in (closed_loop, gains, feedforward, drift_terms, initial_states.T)
        )
    )
    return pl.pallas_call(
        functools.partial(store_kernel, halves),
        out_shape=(
            jax.ShapeDtypeStruct((sl, nx, steps), f32),
            jax.ShapeDtypeStruct((sl, nu, steps), f32),
        ),
        in_specs=[vmem] * 2,
        out_specs=(hbm, hbm),
        scratch_shapes=[dma((2, halves))],
        compiler_params=pltpu.CompilerParams(vmem_limit_bytes=2**20),
    )(x_tile.reshape(halves, sl, nx, LANES), u_tile.reshape(halves, sl, nu, LANES))


def solution(mesh):
    return jax.shard_map(
        body,
        mesh=mesh,
        in_specs=(
            P("tm", None, None),
            P("tm", None, None),
            P("tm", None),
            P("tm", None),
            P(None, ("tm", "scen")),
        ),
        out_specs=(P(("tm", "scen"), None, None), P(("tm", "scen"), None, None)),
        check_vma=False,
    )
```
